8 devices in a mesh: col: 4 (over z, y, x), row: 2 (over core).
Axes of the slice: x: 2, y: 2, z: 1, core: 2. Of those that a mesh axis runs over, the one named last changes fastest.
Arguments:
- t_amp: float32 [1024, 20736], P('row', 'col')
- d_denom: float32 [1024, 20736], P('row', 'col')
- v_oovv: bfloat16 [1024, 20736], P('row', 'col')
- v_vvvv: bfloat16 [20736, 20736], P('row', 'col')
- v_oooo: bfloat16 [1024, 1024], replicated
- w_ovov: bfloat16 [4608, 4608], P(None, 'col')
Outputs:
- output: float32 [4608, 4608], P('row', 'col')
All inputs are finite; a program needn't handle non-finite values.
Results may differ from the reference program's by a relative error of at most 0.001.
Values are sent between devices in bfloat16 or wider.
A program may use at most 1 GiB of HBM per device.

```python
import math
import jax
import jax.numpy as jnp
from jax import lax

O = 32
V = 144


def pair_layout(entry_mat):
    entry_four = entry_mat.reshape(O, O, V, V).transpose(0, 2, 1, 3)
    return entry_four.reshape(O * V, O * V)


def setup_inputs(seed: int = 0) -> dict:
    key_list = jax.random.split(jax.random.key(seed), 6)
    amp_scale = 1.5 / math.sqrt(O * V)
    ladder_scale = math.sqrt(O / V)
    hole_scale = math.sqrt(V / O) / 1.5
    t_amp = amp_scale * jax.random.normal(key_list[0], (O * O, V * V), jnp.float32)
    d_denom = -(1.0 + 2.0 * jax.random.uniform(key_list[1], (O * O, V * V), jnp.float32))
    v_oovv = jax.random.normal(key_list[2], (O * O, V * V), jnp.float32).astype(jnp.bfloat16)

    def vvvv_rows(row_block):
        sub_key = jax.random.fold_in(key_list[3], row_block)
        rows_f32 = ladder_scale * jax.random.normal(sub_key, (V, V * V), jnp.float32)
        return rows_f32.astype(jnp.bfloat16)

    v_vvvv = lax.map(vvvv_rows, jnp.arange(V)).reshape(V * V, V * V)
    v_oooo = (hole_scale * jax.random.normal(key_list[4], (O * O, O * O), jnp.float32)).astype(jnp.bfloat16)
    w_ovov = (jax.random.normal(key_list[5], (O * V, O * V), jnp.float32) / 1.5).astype(jnp.bfloat16)
    return {"t_amp": t_amp, "d_denom": d_denom, "v_oovv": v_oovv, "v_vvvv": v_vvvv, "v_oooo": v_oooo, "w_ovov": w_ovov}


def reference(t_amp, d_denom, v_oovv, v_vvvv, v_oooo, w_ovov):
    t_bf = t_amp.astype(jnp.bfloat16)
    r_ladder = jnp.dot(t_bf, v_vvvv, preferred_element_type=jnp.float32)
    x_inter = jnp.dot(v_oovv, t_bf.T, preferred_element_type=jnp.float32)
    w_hole = (v_oooo.astype(jnp.float32) + 0.5 * x_inter).astype(jnp.bfloat16)
    r_hole = jnp.dot(w_hole.T, t_bf, preferred_element_type=jnp.float32)
    entry_sum = v_oovv.astype(jnp.float32) + r_ladder + r_hole
    t_mixed = pair_layout(t_bf)
    r_mixed = jnp.dot(t_mixed, w_ovov, preferred_element_type=jnp.float32)
    return (pair_layout(entry_sum) + r_mixed + r_mixed.T) / pair_layout(d_denom)
```

```python
import functools
import jax, jax.numpy as jnp
from jax import lax
from jax.experimental import pallas as pl
from jax.experimental.pallas import tpu as pltpu
from jax.sharding import PartitionSpec as P
F32=jnp.float32; BF=jnp.bfloat16
def rl_kernel(x_ref,o_ref,scr,scr2,*,na,pitch):
    @pl.loop(0,na)
    def _(q):
        m=x_ref[q,:128].astype(F32).T
        t=x_ref[q,128:].astype(F32).T
        for i in range(16):
            scr[i*pitch:i*pitch+32]=m[i*32:(i+1)*32]
            scr2[i*pitch:i*pitch+32,:16]=t[i*32:(i+1)*32]
        for j in range(32):
            c,jj=divmod(j,8)
            for g in range(2):
                v=scr[pl.ds(j+g*8*pitch,8,stride=pitch),:]
                v2=scr2[pl.ds(j+g*8*pitch,8,stride=pitch),:]
                o_ref[c,g,q,:,jj*144:jj*144+128]=v
                o_ref[c,g,q,:,jj*144+128:(jj+1)*144]=v2[:,:16]
def rl(x,na=4,pitch=40):
    A=x.shape[0]
    return pl.pallas_call(functools.partial(rl_kernel,na=na,pitch=pitch),grid=(A//na,),
      in_specs=[pl.BlockSpec((na,144,512),lambda i:(i,0,0))],
      out_specs=pl.BlockSpec((4,2,na,8,1152),lambda i:(0,0,i,0,0)),
      out_shape=jax.ShapeDtypeStruct((4,2,A,8,1152),F32),
      scratch_shapes=[pltpu.VMEM((16*pitch,128),F32)]*2)(x)
def tm_kernel(x_ref,o_ref,scr,scr2,*,nb,pitch):
    @pl.loop(0,nb)
    def _(q):
        off=pl.multiple_of(q*pitch,8)
        scr[pl.ds(off,512),:]=x_ref[q,:128].astype(F32).T
        scr2[pl.ds(off,512),:16]=x_ref[q,128:].astype(F32).T
    @pl.loop(0,16)
    def _(j):
        for k in range(32):
            v=scr[pl.ds(j*32+k,nb,stride=pitch),:]
            v2=scr2[pl.ds(j*32+k,nb,stride=pitch),:]
            o_ref[j,:,k*144:k*144+128]=v.astype(o_ref.dtype)
            o_ref[j,:,k*144+128:(k+1)*144]=v2[:,:16].astype(o_ref.dtype)
def tm(x,nb=16,pitch=520):
    A=x.shape[0]
    return pl.pallas_call(functools.partial(tm_kernel,nb=nb,pitch=pitch),grid=(A//nb,),
      in_specs=[pl.BlockSpec((nb,144,512),lambda i:(i,0,0))],
      out_specs=pl.BlockSpec((16,nb,4608),lambda i:(0,i,0)),
      out_shape=jax.ShapeDtypeStruct((16,A,4608),BF),
      scratch_shapes=[pltpu.VMEM((nb*pitch,128),F32)]*2)(x)
def wt_kernel(w_ref,o_ref,scr):
    for h in range(2):
        scr[...]=w_ref[h*128:(h+1)*128].astype(F32).T
        for a in range(0,144,2):
            v=jnp.concatenate([scr[pl.ds(a,8,stride=144),:],scr[pl.ds(a+1,8,stride=144),:]],axis=0)
            o_ref[a*8:a*8+16,h*128:(h+1)*128]=v.astype(o_ref.dtype)
def wt(w):
    K=w.shape[0]
    return pl.pallas_call(wt_kernel,grid=(K//256,),
      in_specs=[pl.BlockSpec((256,1152),lambda i:(i,0))],
      out_specs=pl.BlockSpec((1152,256),lambda i:(0,i)),
      out_shape=jax.ShapeDtypeStruct((1152,K),BF),
      scratch_shapes=[pltpu.VMEM((1152,128),F32)])(w)
def fin_kernel(c_ref,b0,b1,b2,b3,d0,d1,d2,d3,r_ref,o_ref,ns,ds_):
    c=c_ref[0]
    for m,(b,d) in enumerate(((b0,d0),(b1,d1),(b2,d2),(b3,d3))):
        if m==0: b=b.at[0]; d=d.at[0]
        for g in range(2):
            off=pl.multiple_of(g*1152+(c^m)*288,8)
            ns[pl.ds(off,288),:]=b[g].reshape(288,b.shape[-1])
            ds_[pl.ds(off,288),:]=d[g].reshape(288,d.shape[-1])
    @pl.loop(0,8)
    def _(i):
        for g in range(2):
            for a in range(0,144,8):
                n=ns[pl.ds(g*1152+a*8+i,8,stride=8),:]
                q=ds_[pl.ds(g*1152+a*8+i,8,stride=8),:]
                o_ref[g*8+i,a:a+8,:]=(n+r_ref[g*8+i,a:a+8,:])/q
def fin(cidx,base,bs,d,dsx,r3):
    L=128
    own=pl.BlockSpec((1,2,36,8,L),lambda l,c:(c[0],0,0,0,l))
    oth=pl.BlockSpec((2,36,8,L),lambda l,c:(0,0,0,l))
    full=pl.BlockSpec((16,144,L),lambda l,c:(0,0,l))
    return pl.pallas_call(fin_kernel,
      grid_spec=pltpu.PrefetchScalarGridSpec(num_scalar_prefetch=1,grid=(9,),
        in_specs=[own,oth,oth,oth,own,oth,oth,oth,full],out_specs=full,
        scratch_shapes=[pltpu.VMEM((2304,L),F32)]*2),
      out_shape=jax.ShapeDtypeStruct((16,144,1152),F32))(cidx,base,*bs,d,*dsx,r3)

def rla_kernel(s_ref,x_ref,a_ref,b_ref,o_ref,scr,scr2,*,na,pitch):
    own=s_ref[0]
    @pl.loop(0,na)
    def _(q):
        m=x_ref[q,:128].T
        t=x_ref[q,128:].T
        for i in range(16):
            scr[i*pitch:i*pitch+32]=m[i*32:(i+1)*32]
            scr2[i*pitch:i*pitch+32,:16]=t[i*32:(i+1)*32]
        for h in range(2):
            def put(im_ref):
                for jh in range(16):
                    j=h*16+jh
                    c,jj=divmod(j,8)
                    for g in range(2):
                        v=scr[pl.ds(j+g*8*pitch,8,stride=pitch),:]
                        v2=scr2[pl.ds(j+g*8*pitch,8,stride=pitch),:]
                        o_ref[c,g,q,:,jj*144:jj*144+128]=v
                        o_ref[c,g,q,:,jj*144+128:(jj+1)*144]=v2[:,:16]
                for c in range(2):
                    for g in range(2):
                        o_ref[2*h+c,g,q]+=im_ref[g,q,:,c*1152:(c+1)*1152]
            @pl.when(own==h)
            def _(): put(a_ref)
            @pl.when(own!=h)
            def _(): put(b_ref)
def rl_add(s,x,a,b,na=4,pitch=40):
    A=x.shape[0]
    im=pl.BlockSpec((2,na,8,2304),lambda i,s:(0,i,0,0))
    return pl.pallas_call(functools.partial(rla_kernel,na=na,pitch=pitch),
      grid_spec=pltpu.PrefetchScalarGridSpec(num_scalar_prefetch=1,grid=(A//na,),
      in_specs=[pl.BlockSpec((na,144,512),lambda i,s:(i,0,0)),im,im],
      out_specs=pl.BlockSpec((4,2,na,8,1152),lambda i,s:(0,0,i,0,0)),
      scratch_shapes=[pltpu.VMEM((16*pitch,128),F32)]*2),
      out_shape=jax.ShapeDtypeStruct((4,2,A,8,1152),F32))(s,x,a,b)


def solution(mesh):
    row_n = mesh.shape["row"]
    col_n = mesh.shape["col"]
    flip = [(0, 1), (1, 0)]

    def hop(x, m):
        return lax.ppermute(x, "col", [(i, i ^ m) for i in range(col_n)])

    def swap(x):
        return lax.ppermute(x, "row", flip)

    def pick(x, i):
        return lax.dynamic_index_in_dim(x, i, 0, keepdims=False)

    def mm(a, b, dims):
        return lax.dot_general(a, b, (dims, ((), ())), preferred_element_type=F32)

    def local_sweep(t_blk, d_blk, voovv_blk, vvvvv_blk, oooo, w_blk):
        c = lax.axis_index("col")
        r = lax.axis_index("row")
        t_own = t_blk.T.astype(BF)
        d_t, v_t, vv_t = d_blk.T, voovv_blk.T, vvvvv_blk.T
        t_full = lax.all_gather(t_own, "col", axis=0, tiled=True)
        t_cat = jnp.concatenate([t_own, swap(t_own)], axis=1)
        x_part = mm(v_t, t_cat, ((0,), (0,)))
        x_sum = lax.psum(x_part, "col")
        x_oth = swap(x_sum[:, 512:])
        o_own = lax.dynamic_slice(oooo, (r * 512, r * 512), (512, 512))
        o_oth = lax.dynamic_slice(oooo, ((1 - r) * 512, r * 512), (512, 512))
        w_own = (o_own.astype(F32) + 0.5 * x_sum[:, :512]).astype(BF)
        w_oth = (o_oth.astype(F32) + 0.5 * x_oth).astype(BF)
        r2 = mm(t_cat, jnp.concatenate([w_own, w_oth], axis=0), ((1,), (0,)))
        wt_all = wt(w_blk).reshape(4, 2, 144, 4608)
        d_all = rl(d_t.reshape(36, 144, 512))
        wt_all, d_all, t_full = lax.optimization_barrier((wt_all, d_all, t_full))
        got = [hop(pick(pick(wt_all, c ^ m), r), m) for m in (1, 2, 3)]
        oth = swap(jnp.stack(got))
        wimg = jnp.zeros((8, 144, 4608), BF)
        wimg = lax.dynamic_update_slice(wimg, pick(wt_all, c), (2 * c, 0, 0))
        for n, m in enumerate((1, 2, 3)):
            wimg = lax.dynamic_update_slice(wimg, got[n][None], (2 * (c ^ m) + r, 0, 0))
            wimg = lax.dynamic_update_slice(wimg, oth[n][None], (2 * (c ^ m) + 1 - r, 0, 0))
        wimg = wimg.reshape(2, 576, 4608)
        t_snd = lax.dynamic_slice(t_full, ((1 - r) * 10368, 0), (10368, 512))
        t_rcv = swap(t_snd)
        t_mine = lax.dynamic_slice(t_full, (r * 10368, 0), (10368, 512))
        r1_oth = swap(mm(vv_t, t_rcv, ((1,), (0,))))
        r1_own = mm(vv_t, t_mine, ((1,), (0,)))
        tmix = tm(t_full.reshape(144, 144, 512)).reshape(2304, 4608)
        im_oth = swap(mm(pick(wimg, 1 - r), tmix, ((1,), (1,))))
        im_own = mm(pick(wimg, r), tmix, ((1,), (1,)))
        base = r1_own + r1_oth + (r2 + v_t.astype(F32))
        b_all = rl_add(r.reshape(1), base.reshape(36, 144, 512), im_own.reshape(2, 36, 8, 2304), im_oth.reshape(2, 36, 8, 2304))
        d_got = [hop(pick(d_all, c ^ m), m) for m in (1, 2, 3)]
        b_got = [hop(pick(b_all, c ^ m), m) for m in (1, 2, 3)]
        r3 = mm(tmix, w_blk, ((1,), (0,))).reshape(16, 144, 1152)
        out = fin(c.reshape(1), b_all, b_got, d_all, d_got, r3)
        return out.reshape(2304, 1152)

    return jax.shard_map(
        local_sweep,
        mesh=mesh,
        in_specs=(P("row", "col"), P("row", "col"), P("row", "col"), P("row", "col"), P(None, None), P(None, "col")),
        out_specs=P("row", "col"),
        check_vma=False,
    )
```

```python
import functools
import jax
import jax.numpy as jnp
from jax import lax
from jax.experimental import pallas as pl
from jax.experimental.pallas import tpu as pltpu
from jax.sharding import PartitionSpec as P


F32 = jnp.float32
BF = jnp.bfloat16


def cost(nbytes, us):
    return pl.CostEstimate(flops=int(us * 6e7), bytes_accessed=nbytes, transcendentals=0)


def put_rows(x, scr, scr2, n_i, pitch):
    m, t = x[:128].T, x[128:].T
    for i in range(n_i):
        scr[i * pitch : i * pitch + 32] = m[i * 32 : (i + 1) * 32]
        scr2[i * pitch : i * pitch + 32, :16] = t[i * 32 : (i + 1) * 32]


def d_kernel(x_ref, o_ref, scr, scr2, *, na, pitch):
    @pl.loop(0, na)
    def _(q):
        put_rows(x_ref[q], scr, scr2, 16, pitch)
        for j in range(32):
            c, jj = divmod(j, 8)
            for g in range(2):
                rows = pl.ds(j + g * 8 * pitch, 8, stride=pitch)
                o_ref[c, g, q, :, jj * 144 : jj * 144 + 128] = scr[rows, :]
                o_ref[c, g, q, :, jj * 144 + 128 : (jj + 1) * 144] = scr2[rows, :][:, :16]


def regroup_d(x, na=4, pitch=40):
    return pl.pallas_call(
        functools.partial(d_kernel, na=na, pitch=pitch),
        grid=(36 // na,),
        in_specs=[pl.BlockSpec((na, 144, 512), lambda i: (i, 0, 0))],
        out_specs=pl.BlockSpec((4, 2, na, 8, 1152), lambda i: (0, 0, i, 0, 0)),
        out_shape=jax.ShapeDtypeStruct((4, 2, 36, 8, 1152), F32),
        scratch_shapes=[pltpu.VMEM((16 * pitch, 128), F32)] * 2,
        cost_estimate=cost(2 * 10616832, 17),
    )(x)


def base_kernel(s_ref, p_ref, q_ref, v_ref, al, ah, bl, bh, o_ref, scr, scr2, *, na, pitch):
    own = s_ref[0]

    @pl.loop(0, na)
    def _(q):
        put_rows(p_ref[q] + q_ref[q] + v_ref[q], scr, scr2, 8, pitch)
        for j in range(32):
            c, jj = divmod(j, 8)
            rows = pl.ds(j, 8, stride=pitch)
            o_ref[c, q, :, jj * 144 : jj * 144 + 128] = scr[rows, :]
            o_ref[c, q, :, jj * 144 + 128 : (jj + 1) * 144] = scr2[rows, :][:, :16]
        for c in range(4):
            pair = ((al, bl), (ah, bh))[c % 2]

            @pl.when(own == c // 2)
            def _():
                o_ref[c, q] += pair[0][0, 0, q]

            @pl.when(own != c // 2)
            def _():
                o_ref[c, q] += pair[1][0, 0, q]


def regroup_base(g, s, p, q, v, imgs, na=4, pitch=40):
    own = pl.BlockSpec((1, 1, na, 8, 1152), lambda i, s: (s[0], g, i, 0, 0))
    im = pl.BlockSpec((1, 1, na, 8, 1152), lambda i, s: (0, g, i, 0, 0))
    return pl.pallas_call(
        functools.partial(base_kernel, na=na, pitch=pitch),
        grid_spec=pltpu.PrefetchScalarGridSpec(
            num_scalar_prefetch=1,
            grid=(36 // na,),
            in_specs=[
                pl.BlockSpec((na, 144, 256), lambda i, s: (i, 0, 0)),
                pl.BlockSpec((na, 144, 256), lambda i, s: (i, 0, 1)),
                pl.BlockSpec((na, 144, 256), lambda i, s: (i, 0, g)),
                own, own, im, im,
            ],
            out_specs=pl.BlockSpec((4, na, 8, 1152), lambda i, s: (0, i, 0, 0)),
            scratch_shapes=[pltpu.VMEM((8 * pitch, 128), F32)] * 2,
        ),
        out_shape=jax.ShapeDtypeStruct((4, 36, 8, 1152), F32),
        cost_estimate=cost(5 * 5308416, 16),
    )(s, p, q, v, *imgs)


def mix_kernel(x_ref, *rest, nb, nj, pitch):
    o_ref, scr, scr2 = rest[-3:]

    @pl.loop(0, nb)
    def _(q):
        rows = pl.ds(pl.multiple_of(q * pitch, 8), nj * 32)
        scr[rows, :] = x_ref[q, :128].T.astype(F32)
        scr2[rows, :16] = x_ref[q, 128:].T.astype(F32)

    @pl.loop(0, nj)
    def _(j):
        for k in range(32):
            rows = pl.ds(j * 32 + k, nb, stride=pitch)
            o_ref[j, :, k * 144 : k * 144 + 128] = scr[rows, :].astype(BF)
            o_ref[j, :, k * 144 + 128 : (k + 1) * 144] = scr2[rows, :][:, :16].astype(BF)


def mix(x, part=0, prev=None, nb=16):
    nj = x.shape[-1] // 32
    pitch = nj * 32 + 8
    in_specs = [pl.BlockSpec((nb, 144, nj * 32), lambda i: (i, 0, 0))]
    args, alias = [x], {}
    if prev is not None:
        in_specs += [pl.BlockSpec(memory_space=pl.ANY)]
        args, alias = [x, prev], {1: 0}
    return pl.pallas_call(
        functools.partial(mix_kernel, nb=nb, nj=nj, pitch=pitch),
        grid=(144 // nb,),
        in_specs=in_specs,
        out_specs=pl.BlockSpec((nj, nb, 4608), lambda i: (part, i, 0)),
        out_shape=jax.ShapeDtypeStruct((8, 144, 4608), BF),
        scratch_shapes=[pltpu.VMEM((nb * pitch, 128), F32)] * 2,
        input_output_aliases=alias,
        cost_estimate=cost(nj * 2654208, nj * 3.6),
    )(*args)


def wt_kernel(w_ref, o_ref, scr):
    for h in range(2):
        scr[...] = w_ref[h * 128 : (h + 1) * 128].astype(F32).T
        for a in range(0, 144, 2):
            v = jnp.concatenate([scr[pl.ds(a, 8, stride=144), :], scr[pl.ds(a + 1, 8, stride=144), :]], axis=0)
            o_ref[a * 8 : a * 8 + 16, h * 128 : (h + 1) * 128] = v.astype(BF)


def w_rows(w):
    return pl.pallas_call(
        wt_kernel,
        grid=(18,),
        in_specs=[pl.BlockSpec((256, 1152), lambda i: (i, 0))],
        out_specs=pl.BlockSpec((1152, 256), lambda i: (0, i)),
        out_shape=jax.ShapeDtypeStruct((1152, 4608), BF),
        scratch_shapes=[pltpu.VMEM((1152, 128), F32)],
        cost_estimate=cost(2 * 10616832, 19),
    )(w)


def place_kernel(s_ref, *refs):
    o_ref = refs[-1]
    for n in range(8):
        @pl.when(pl.program_id(0) == n)
        def _():
            o_ref[0] = refs[n].at[0][...]


def place(idx, own, got, oth):
    def one(f):
        return pl.BlockSpec((1, 144, 4608), f)

    specs = [one(lambda n, s: (2 * s[8], 0, 0)), one(lambda n, s: (2 * s[8] + 1, 0, 0))]
    specs += [one(lambda n, s: (0, 0, 0))] * 6
    return pl.pallas_call(
        place_kernel,
        grid_spec=pltpu.PrefetchScalarGridSpec(
            num_scalar_prefetch=1,
            grid=(8,),
            in_specs=specs,
            out_specs=pl.BlockSpec((1, 144, 4608), lambda n, s: (s[n], 0, 0)),
        ),
        out_shape=jax.ShapeDtypeStruct((8, 144, 4608), BF),
        cost_estimate=cost(2 * 10616832, 8),
    )(idx, own, own, *got, *oth)


def fin_kernel(c_ref, b0, b1, b2, b3, d0, d1, d2, d3, r_ref, *rest):
    o_ref, ns, ds = rest[-3:]
    c = c_ref[0]
    lanes = o_ref.shape[-1]
    for m, (b, d) in enumerate(((b0, d0.at[0, 0]), (b1, d1.at[0]), (b2, d2.at[0]), (b3, d3.at[0]))):
        rows = pl.ds(pl.multiple_of((c ^ m) * 288, 8), 288)
        ns[rows, :] = b[...].reshape(288, lanes)
        ds[rows, :] = d[...].reshape(288, lanes)

    @pl.loop(0, 8)
    def _(i):
        for a in range(0, 144, 8):
            rows = pl.ds(a * 8 + i, 8, stride=8)
            o_ref[i, a : a + 8, :] = (ns[rows, :] + r_ref[i, a : a + 8, :]) / ds[rows, :]


def finish(g, cidx, b_own, b_got, d_all, d_got, r3, prev=None, lanes=128):
    in_specs = [pl.BlockSpec((36, 8, lanes), lambda l, c: (0, 0, l))] * 4
    in_specs += [pl.BlockSpec((1, 1, 36, 8, lanes), lambda l, c: (c[0], g, 0, 0, l))]
    in_specs += [pl.BlockSpec((1, 36, 8, lanes), lambda l, c: (g, 0, 0, l))] * 3
    in_specs += [pl.BlockSpec((8, 144, lanes), lambda l, c: (0, 0, l))]
    args = [cidx, b_own, *b_got, d_all, *d_got, r3]
    alias = {}
    if prev is not None:
        in_specs += [pl.BlockSpec(memory_space=pl.ANY)]
        alias = {len(args): 0}
        args += [prev]
    return pl.pallas_call(
        fin_kernel,
        grid_spec=pltpu.PrefetchScalarGridSpec(
            num_scalar_prefetch=1,
            grid=(1152 // lanes,),
            in_specs=in_specs,
            out_specs=pl.BlockSpec((8, 144, lanes), lambda l, c: (g, 0, l)),
            scratch_shapes=[pltpu.VMEM((1152, lanes), F32)] * 2,
        ),
        out_shape=jax.ShapeDtypeStruct((16, 144, 1152), F32),
        input_output_aliases=alias,
        cost_estimate=cost(4 * 5308416, 10),
    )(*args)


def solution(mesh):
    col_n = mesh.shape["col"]
    flip = [(0, 1), (1, 0)]

    def hop(x, m):
        return lax.ppermute(x, "col", [(i, i ^ m) for i in range(col_n)])

    def swap(x):
        return lax.ppermute(x, "row", flip)

    def pick(x, i):
        return lax.dynamic_index_in_dim(x, i, 0, keepdims=False)

    def mm(a, b, dims):
        return lax.dot_general(a, b, (dims, ((), ())), preferred_element_type=F32)

    fence = lax.optimization_barrier

    def sweep(t_blk, d_blk, voovv_blk, vvvvv_blk, oooo, w_blk):
        c = lax.axis_index("col")
        r = lax.axis_index("row")
        t_own = t_blk.T.astype(BF)
        d_t, v_t, vv_t = d_blk.T, voovv_blk.T, vvvvv_blk.T
        gather = functools.partial(lax.all_gather, axis_name="col", axis=0, tiled=True)
        t_a = gather(t_own[:, :128])
        t_b = gather(t_own[:, 128:256])
        t_hi = gather(t_own[:, 256:])
        t_cat = jnp.concatenate([t_own, swap(t_own)], axis=1)
        x_part = mm(v_t, t_cat, ((0,), (0,))).reshape(4, 128, 1024)
        wt_all = w_rows(w_blk).reshape(8, 144, 4608)
        d_all = regroup_d(d_t.reshape(36, 144, 512))

        def half(t, who):
            return lax.dynamic_slice(t, (who * 10368, 0), (10368, t.shape[1]))

        x_out = [pick(x_part, c ^ m) for m in range(4)]
        w_out = [pick(wt_all, 2 * (c ^ m) + r) for m in (1, 2, 3)]
        d_out = [pick(d_all, c ^ m) for m in (1, 2, 3)]
        t_a, w_out, d_out, x_out = fence((t_a, w_out, d_out, x_out))
        s_a = swap(half(t_a, 1 - r))
        mix_lo = mix(t_a.reshape(144, 144, 128))
        t_b, x_out, mix_lo = fence((t_b, x_out, mix_lo))
        x_got = [hop(x_out[m], m) for m in (1, 2, 3)]
        s_b = swap(half(t_b, 1 - r))
        mix_lo = mix(t_b.reshape(144, 144, 128), 1, mix_lo).reshape(1152, 4608)
        x_sum = x_out[0] + x_got[0] + x_got[1] + x_got[2]
        o_rows = lax.dynamic_slice(oooo, (r * 512 + c * 128, 0), (128, 1024))
        o_own = lax.dynamic_slice(o_rows, (0, r * 512), (128, 512))
        o_oth = lax.dynamic_slice(o_rows, (0, (1 - r) * 512), (128, 512))
        o_rows = jnp.concatenate([o_own, o_oth], axis=1)
        w_sub = (o_rows.astype(F32) + 0.5 * x_sum).astype(BF)
        w_got = [w_sub] + [hop(w_sub, m) for m in (1, 2, 3)]
        w_hole = []
        for n in range(4):
            sel = jnp.where(c ^ n == 2, w_got[2], w_got[3])
            w_hole.append(jnp.where(c ^ n == 0, w_got[0], jnp.where(c ^ n == 1, w_got[1], sel)))
        w_hole = jnp.concatenate(w_hole, axis=0)
        rhs_lo = jnp.concatenate([half(t_a, r), half(t_b, r), s_a, s_b], axis=1)
        p_lo = mm(vv_t, rhs_lo, ((1,), (0,)))
        w_both = jnp.concatenate([w_hole[:, :512], swap(w_hole[:, 512:])], axis=0)
        r2v = mm(t_cat, w_both, ((1,), (0,))) + v_t.astype(F32)
        q_lo = swap(p_lo)
        t_hi, w_out, d_out, p_lo = fence((t_hi, w_out, d_out, p_lo))
        w_got = [hop(x, m) for m, x in enumerate(w_out, 1)]
        d_got = [hop(x, m) for m, x in enumerate(d_out, 1)]
        s_hi = swap(half(t_hi, 1 - r))
        mix_hi = mix(t_hi.reshape(144, 144, 256)).reshape(1152, 4608)
        rhs_hi = jnp.concatenate([half(t_hi, r), s_hi], axis=1)
        p_hi = mm(vv_t, rhs_hi, ((1,), (0,)))
        q_hi = swap(p_hi)
        w_oth = [swap(x) for x in w_got]
        idx = jnp.stack([2 * c, 2 * c + 1] + [2 * (c ^ m) + r for m in (1, 2, 3)] + [2 * (c ^ m) + 1 - r for m in (1, 2, 3)] + [c])
        w_img = place(idx, wt_all, [x[None] for x in w_got], [x[None] for x in w_oth]).reshape(1152, 4608)
        im_lo = mm(w_img, mix_lo, ((1,), (1,))).reshape(2, 2, 36, 8, 1152)
        im_hi = mm(w_img, mix_hi, ((1,), (1,))).reshape(2, 2, 36, 8, 1152)
        imgs = [im_lo, im_hi, swap(pick(im_lo, 1 - r))[None], swap(pick(im_hi, 1 - r))[None]]
        shape = (36, 144, 512)
        rv = r.reshape(1)
        r2v = r2v.reshape(shape)
        b_lo = regroup_base(0, rv, p_lo.reshape(shape), q_lo.reshape(shape), r2v, imgs)
        b_lo = [pick(b_lo, c ^ m) for m in range(4)]
        lo_got = [hop(b_lo[m], m) for m in (1, 2, 3)]
        b_hi = regroup_base(1, rv, p_hi.reshape(shape), q_hi.reshape(shape), r2v, imgs)
        b_hi = [pick(b_hi, c ^ m) for m in range(4)]
        hi_got = [hop(b_hi[m], m) for m in (1, 2, 3)]
        r3_lo = mm(mix_lo, w_blk, ((1,), (0,))).reshape(8, 144, 1152)
        r3_hi = mm(mix_hi, w_blk, ((1,), (0,))).reshape(8, 144, 1152)
        cv = c.reshape(1)
        out = finish(0, cv, b_lo[0], lo_got, d_all, d_got, r3_lo)
        out = finish(1, cv, b_hi[0], hi_got, d_all, d_got, r3_hi, out)
        return out.reshape(2304, 1152)

    return jax.shard_map(
        sweep,
        mesh=mesh,
        in_specs=(P("row", "col"), P("row", "col"), P("row", "col"), P("row", "col"), P(None, None), P(None, "col")),
        out_specs=P("row", "col"),
        check_vma=False,
    )
```
